8 devices in a mesh: data: 1 (over z), seq: 2 (over y), dap: 4 (over x, core).
Axes of the slice: x: 2, y: 2, z: 1, core: 2. Of those that a mesh axis runs over, the one named last changes fastest.
Arguments:
- msa_act: bfloat16 [256, 384, 64], P(('data', 'seq', 'dap'))
- msa_mask: int32 [256, 384], P(('data', 'seq', 'dap'))
- pair_act: float32 [384, 384, 128], P(('data', 'dap'))
- ln_gamma: bfloat16 [64], replicated
- ln_beta: bfloat16 [64], replicated
- w_a: bfloat16 [64, 32], replicated
- b_a: bfloat16 [32], replicated
- w_b: bfloat16 [64, 32], replicated
- b_b: bfloat16 [32], replicated
- w_out: bfloat16 [1024, 128], replicated
- b_out: bfloat16 [128], replicated
Outputs:
- output: float32 [384, 384, 128], P(('data', 'dap'))
All inputs are finite; a program needn't handle non-finite values.
Results may differ from the reference program's by a relative error of at most 0.00769173.
Values are sent between devices in bfloat16 or wider.
A program may use at most 1 GiB of HBM per device.

```python
import jax
import jax.numpy as jnp
from jax import lax

NUM_SEQS = 256
NUM_RES = 384
MSA_DIM = 64
PAIR_DIM = 128
HIDDEN = 32
SEQ_BLOCK = 8


def draw_mask(level_key, draw_key):
    levels = jax.random.randint(level_key, (NUM_SEQS, 1), 0, 17)
    draws = jax.random.randint(draw_key, (NUM_SEQS, NUM_RES), 0, 16)
    first_row = (jnp.arange(NUM_SEQS) == 0)[:, None]
    return jnp.where(first_row | (draws < levels), 1, 0).astype(jnp.int32)


def setup_inputs(seed: int = 0, part: int = 0) -> dict:
    root = jax.random.key(seed)
    shared = jax.random.split(root, 8)
    own = jax.random.split(jax.random.fold_in(root, part), 4)
    common = NUM_SEQS ** -0.25

    def normal(key, shape):
        return jax.random.normal(key, shape, jnp.float32)

    msa_act = normal(own[0], (NUM_SEQS, NUM_RES, MSA_DIM)).astype(jnp.bfloat16)
    msa_mask = draw_mask(own[1], own[2])
    pair_act = normal(own[3], (NUM_RES, NUM_RES, PAIR_DIM))
    ln_gamma = (1.0 + 0.5 * normal(shared[0], (MSA_DIM,))).astype(jnp.bfloat16)
    ln_beta = (0.7 * common * normal(shared[1], (MSA_DIM,))).astype(jnp.bfloat16)
    w_a = (normal(shared[2], (MSA_DIM, HIDDEN)) * MSA_DIM ** -0.5).astype(jnp.bfloat16)
    b_a = (0.7 * common * normal(shared[3], (HIDDEN,))).astype(jnp.bfloat16)
    w_b = (normal(shared[4], (MSA_DIM, HIDDEN)) * MSA_DIM ** -0.5).astype(jnp.bfloat16)
    b_b = (0.7 * common * normal(shared[5], (HIDDEN,))).astype(jnp.bfloat16)
    w_out = (normal(shared[6], (HIDDEN * HIDDEN, PAIR_DIM)) * (0.7 * NUM_SEQS ** 0.5 / HIDDEN)).astype(jnp.bfloat16)
    b_out = (0.5 * NUM_SEQS * normal(shared[7], (PAIR_DIM,))).astype(jnp.bfloat16)
    return {'msa_act': msa_act, 'msa_mask': msa_mask, 'pair_act': pair_act, 'ln_gamma': ln_gamma, 'ln_beta': ln_beta, 'w_a': w_a, 'b_a': b_a, 'w_b': w_b, 'b_b': b_b, 'w_out': w_out, 'b_out': b_out}


def layer_norm(msa_blk, ln_gamma, ln_beta):
    values = msa_blk.astype(jnp.float32)
    row_mean = jnp.mean(values, axis=-1, keepdims=True)
    centered = values - row_mean
    variance = jnp.mean(centered * centered, axis=-1, keepdims=True)
    normed = centered * lax.rsqrt(variance + 1e-5)
    return (normed * ln_gamma.astype(jnp.float32) + ln_beta.astype(jnp.float32)).astype(jnp.bfloat16)


def project(normed, weight, bias_vec, weight_mask):
    summed = jnp.einsum('snk,kc->snc', normed.astype(jnp.float32), weight.astype(jnp.float32))
    return ((summed + bias_vec.astype(jnp.float32)) * weight_mask[..., None]).astype(jnp.bfloat16)


def reference(msa_act, msa_mask, pair_act, ln_gamma, ln_beta, w_a, b_a, w_b, b_b, w_out, b_out):
    w_cube = w_out.astype(jnp.float32).reshape(HIDDEN, HIDDEN, PAIR_DIM)
    num_blocks = NUM_SEQS // SEQ_BLOCK
    msa_blocks = msa_act.reshape(num_blocks, SEQ_BLOCK, NUM_RES, MSA_DIM)
    mask_blocks = msa_mask.reshape(num_blocks, SEQ_BLOCK, NUM_RES)

    def body(carry, block_in):
        sum_r, sum_n = carry
        msa_blk, mask_blk = block_in
        seq_keep = mask_blk.astype(jnp.float32)
        normed = layer_norm(msa_blk, ln_gamma, ln_beta)
        left = project(normed, w_a, b_a, seq_keep)
        right = project(normed, w_b, b_b, seq_keep)
        lifted = jnp.einsum('sic,cde->side', left.astype(jnp.float32), w_cube).astype(jnp.bfloat16)
        sum_r = sum_r + jnp.einsum('side,sjd->ije', lifted.astype(jnp.float32), right.astype(jnp.float32))
        sum_n = sum_n + jnp.einsum('si,sj->ij', seq_keep, seq_keep)
        return (sum_r, sum_n), None

    start_state = (jnp.zeros((NUM_RES, NUM_RES, PAIR_DIM), jnp.float32), jnp.zeros((NUM_RES, NUM_RES), jnp.float32))
    (total_r, total_n), _ = lax.scan(body, start_state, (msa_blocks, mask_blocks))
    return pair_act + (total_r + b_out.astype(jnp.float32)) / (1e-3 + total_n[..., None])
```

```python
import functools

import jax
import jax.numpy as jnp
from jax import lax
from jax.experimental import pallas as pl
from jax.experimental.pallas import tpu as pltpu
from jax.sharding import PartitionSpec as P

MESH = pl.DeviceIdType.MESH
S_LOC, N, K, C, E = 32, 384, 64, 32, 128
S = 256
ROWS = 96
JC = 3
CG = 8
D_VIA_X = 24
IB = 8


def exchange_kernel(x_ref, mask_ref, par_ref, wt_ref, wo_ref,
                    at_ref, ball_ref, inv_ref, wot_ref,
                    stage, ta, ra, rp, mall, atf, wof, ns, ssem, rsem):
    y = lax.axis_index('seq')
    r = lax.axis_index('dap')
    x = r // 2
    c = r % 2
    me = y * 4 + r
    dev_x = (0, y, (1 - x) * 2 + c)
    dev_y = (0, 1 - y, r)
    dev_p = (0, y, x * 2 + 1 - c)
    id_x = y * 4 + (1 - x) * 2 + c
    id_y = (1 - y) * 4 + r
    id_xy = (1 - y) * 4 + (1 - x) * 2 + c
    id_p = y * 4 + x * 2 + 1 - c

    barrier = pltpu.get_barrier_semaphore()
    flips = [(fy, fr) for fy in range(2) for fr in range(4) if fy or fr]
    for fy, fr in flips:
        peer = (0, (y + fy) % 2, (r + fr) % 4)
        pl.semaphore_signal(barrier, inc=1, device_id=peer, device_id_type=MESH)

    gamma, beta, bias = par_ref[:, 0:1], par_ref[:, 1:2], par_ref[:, 2:3]
    wt = wt_ref[...]

    def one_seq(s, carry):
        v = x_ref[s].astype(jnp.float32)
        mean = jnp.sum(v, axis=0, keepdims=True) * (1.0 / K)
        cen = v - mean
        var = jnp.sum(cen * cen, axis=0, keepdims=True) * (1.0 / K)
        xn = (cen * lax.rsqrt(var + 1e-5) * gamma + beta).astype(jnp.bfloat16)
        out = jnp.dot(wt, xn, preferred_element_type=jnp.float32)
        keep = mask_ref[pl.ds(s, 1), :].astype(jnp.float32)
        out = (out + bias) * keep
        for t in range(3):
            stage[t, pl.ds(s, 2 * C, stride=S_LOC), :] = out[:, t * 128:(t + 1) * 128]
        return carry

    lax.fori_loop(0, S_LOC, one_seq, 0, unroll=4)

    my_rows = pl.ds(pl.multiple_of(me * S_LOC, S_LOC), S_LOC)

    for g in range(CG):
        for t in range(3):
            blk = stage[t, g * 128:(g + 1) * 128, :]
            blk = blk.T.astype(jnp.bfloat16)
            lo = t * 128
            while lo < (t + 1) * 128:
                q = lo // ROWS
                hi = min((q + 1) * ROWS, (t + 1) * 128)
                ta[q, g, lo - q * ROWS:hi - q * ROWS, :] = blk[lo - t * 128:hi - t * 128, :]
                lo = hi
    for d in range(C):
        for t in range(JC):
            row = stage[t, (C + d) * S_LOC:(C + d + 1) * S_LOC, :]
            ball_ref[t, d, my_rows, :] = row.astype(jnp.bfloat16)
    mall[my_rows, :] = mask_ref[...].astype(jnp.float32).astype(jnp.bfloat16)

    pl.semaphore_wait(barrier, 7)

    sends = []

    def copy(src, dst, k, dev):
        return pltpu.make_async_remote_copy(
            src_ref=src, dst_ref=dst, send_sem=ssem.at[k], recv_sem=rsem.at[k],
            device_id=dev, device_id_type=MESH)

    def send(src, dst, k, dev):
        cp = copy(src, dst, k, dev)
        cp.start()
        sends.append(cp)

    def arrived(ref, k):
        copy(ref, ref, k, dev_p).wait_recv()

    def rows_of(dev_id):
        return pl.ds(pl.multiple_of(dev_id * S_LOC, S_LOC), S_LOC)

    def b_part(t, dev_id, lo=0, hi=C):
        return ball_ref.at[t, pl.ds(lo, hi - lo), rows_of(dev_id), :]

    A_X, A_Y, A_XY = 0, 1, 2
    A_P = {'o': 3, 'x': 4, 'y': 5, 'd': 6}
    M0 = 7

    def bk(t, what):
        return 14 + t * 9 + ['x', 'y', 'dx', 'dy', 'po', 'px', 'py', 'pdx', 'pdy'].index(what)

    own = 2 * x
    other = 2 * (1 - x)
    send(ta.at[pl.ds(other, 2)], ra.at[0], A_X, dev_x)
    send(ta.at[pl.ds(own, 2)], ra.at[1], A_Y, dev_y)
    send(ta.at[own + 1 - c], rp.at[0], A_P['o'], dev_p)
    for n, (fy, fr) in enumerate(flips):
        peer = (0, (y + fy) % 2, (r + fr) % 4)
        send(mall.at[my_rows], mall.at[my_rows], M0 + n, peer)

    def send_own(t, to):
        dev = {'x': dev_x, 'y': dev_y, 'po': dev_p}[to]
        send(b_part(t, me), b_part(t, me), bk(t, to), dev)

    send_own(0, 'x')
    send_own(0, 'po')

    wof[...] = wo_ref[...].astype(jnp.float32)
    for g in range(CG):
        parts = [wof[pl.ds(4 * g + k, C, stride=C), :] for k in range(4)]
        blk = jnp.concatenate(parts, axis=0)
        wot_ref[:, g * 128:(g + 1) * 128] = blk.T.astype(jnp.bfloat16)

    def got_b(t, frm):
        if frm == 'x':
            arrived(b_part(t, id_x), bk(t, 'x'))
            send(b_part(t, id_x, D_VIA_X, C), b_part(t, id_x, D_VIA_X, C), bk(t, 'dy'), dev_y)
            send(b_part(t, id_x), b_part(t, id_x), bk(t, 'px'), dev_p)
        elif frm == 'y':
            arrived(b_part(t, id_y), bk(t, 'y'))
            send(b_part(t, id_y, 0, D_VIA_X), b_part(t, id_y, 0, D_VIA_X), bk(t, 'dx'), dev_x)
            send(b_part(t, id_y), b_part(t, id_y), bk(t, 'py'), dev_p)
        elif frm == 'dx':
            ref = b_part(t, id_xy, 0, D_VIA_X)
            arrived(ref, bk(t, 'dx'))
            send(ref, ref, bk(t, 'pdx'), dev_p)
        else:
            ref = b_part(t, id_xy, D_VIA_X, C)
            arrived(ref, bk(t, 'dy'))
            send(ref, ref, bk(t, 'pdy'), dev_p)

    arrived(ra.at[0], A_X)
    send(ra.at[0], ra.at[2], A_XY, dev_y)
    send(ra.at[0, 1 - c], rp.at[1], A_P['x'], dev_p)
    send_own(0, 'y')
    send_own(1, 'x')
    arrived(ra.at[1], A_Y)
    send(ra.at[1, 1 - c], rp.at[2], A_P['y'], dev_p)
    got_b(0, 'x')
    send_own(1, 'y')
    send_own(1, 'po')
    send_own(2, 'x')
    arrived(ra.at[2], A_XY)
    send(ra.at[2, 1 - c], rp.at[3], A_P['d'], dev_p)
    got_b(0, 'y')
    send_own(2, 'y')
    send_own(2, 'po')
    for k, name in enumerate(['o', 'x', 'y', 'd']):
        arrived(rp.at[k], A_P[name])

    lane = lax.broadcasted_iota(jnp.int32, (ROWS, 128), 1)
    low = lane < 64
    odd = lax.rem(lane // 32, 2) == 1

    for half in range(2):
        for g in range(CG):
            v = []
            for q in range(4):
                sx, sc = q // 2, q % 2
                same_c = sc == c
                dx = (sx != x).astype(jnp.int32)
                dy = (half != y).astype(jnp.int32)
                slot = dx + 2 * dy
                own_v = ta[r, g].astype(jnp.float32)
                ra_slot = jnp.maximum(slot - 1, 0)
                in_plane = jnp.where(slot == 0, own_v, ra[ra_slot, c, g].astype(jnp.float32))
                v.append(jnp.where(same_c, in_plane, rp[slot, g].astype(jnp.float32)))
            r0, r1, r2, r3 = [pltpu.roll(u, 64, 1) for u in v]
            n0 = jnp.where(low, v[0], r2)
            n1 = jnp.where(low, v[1], r3)
            n2 = jnp.where(low, r0, v[2])
            n3 = jnp.where(low, r1, v[3])
            w0 = jnp.where(odd, pltpu.roll(n1, 32, 1), n0)
            w1 = jnp.where(odd, n1, pltpu.roll(n0, 96, 1))
            w2 = jnp.where(odd, pltpu.roll(n3, 32, 1), n2)
            w3 = jnp.where(odd, n3, pltpu.roll(n2, 96, 1))
            for k, w in enumerate((w0, w1, w2, w3)):
                atf[half, pl.ds(4 * g + k, ROWS, stride=C), :] = w
    for blk in range(12):
        for half in range(2):
            at_ref[blk * 256:(blk + 1) * 256, half * 128:(half + 1) * 128] = (
                atf[half, blk * 256:(blk + 1) * 256, :].astype(jnp.bfloat16))

    got_b(1, 'x')
    got_b(1, 'y')
    got_b(0, 'dx')
    got_b(0, 'dy')
    got_b(2, 'x')
    got_b(2, 'y')

    for n, (fy, fr) in enumerate(flips):
        frm = ((y - fy + 2) % 2) * 4 + (r - fr + 4) % 4
        arrived(mall.at[rows_of(frm)], M0 + n)
    m = mall[...]
    ns[...] = lax.dot_general(m, m, (((0,), (0,)), ((), ())), preferred_element_type=jnp.float32)
    inv_ref[...] = 1.0 / (1e-3 + ns[pl.ds(pl.multiple_of(r * ROWS, ROWS), ROWS), :])

    for t in (1, 2):
        got_b(t, 'dx')
        got_b(t, 'dy')
    id_px = y * 4 + (1 - x) * 2 + 1 - c
    id_py = (1 - y) * 4 + x * 2 + 1 - c
    id_pd = (1 - y) * 4 + (1 - x) * 2 + 1 - c
    for t in range(JC):
        arrived(b_part(t, id_p), bk(t, 'po'))
        arrived(b_part(t, id_px), bk(t, 'px'))
        arrived(b_part(t, id_py), bk(t, 'py'))
        arrived(b_part(t, id_pd, 0, D_VIA_X), bk(t, 'pdx'))
        arrived(b_part(t, id_pd, D_VIA_X, C), bk(t, 'pdy'))
    for cp in sends:
        cp.wait_send()


def exchange(xt, mask, par, wt, w_out):
    vm = pl.BlockSpec(memory_space=pltpu.VMEM)
    nsem = 14 + 9 * JC
    return pl.pallas_call(
        exchange_kernel,
        out_shape=(
            jax.ShapeDtypeStruct((ROWS * C, S), jnp.bfloat16),
            jax.ShapeDtypeStruct((JC, C, S, 128), jnp.bfloat16),
            jax.ShapeDtypeStruct((ROWS, N), jnp.float32),
            jax.ShapeDtypeStruct((E, C * C), jnp.bfloat16),
        ),
        in_specs=[vm] * 5,
        out_specs=(vm,) * 4,
        scratch_shapes=[
            pltpu.VMEM((3, 2 * C * S_LOC, 128), jnp.float32),
            pltpu.VMEM((4, CG, ROWS, 128), jnp.bfloat16),
            pltpu.VMEM((3, 2, CG, ROWS, 128), jnp.bfloat16),
            pltpu.VMEM((4, CG, ROWS, 128), jnp.bfloat16),
            pltpu.VMEM((S, N), jnp.bfloat16),
            pltpu.VMEM((2, ROWS * C, 128), jnp.float32),
            pltpu.VMEM((C * C, E), jnp.float32),
            pltpu.VMEM((N, N), jnp.float32),
            pltpu.SemaphoreType.DMA((nsem,)),
            pltpu.SemaphoreType.DMA((nsem,)),
        ],
        compiler_params=pltpu.CompilerParams(
            collective_id=0, has_side_effects=True, vmem_limit_bytes=60 * 1024 * 1024),
        name='exchange',
    )(xt, mask, par, wt, w_out)


def form_kernel(at_ref, ball_ref, inv_ref, wot_ref, bo_ref, z_ref, out_ref, hi_ref, lo_ref):
    at = at_ref[...]
    for p in range(C // 2):
        rhs = jnp.concatenate([ball_ref[0, 2 * p], ball_ref[0, 2 * p + 1]], axis=1)
        o = jnp.dot(at, rhs, preferred_element_type=jnp.float32)
        hi = o.astype(jnp.bfloat16)
        lo = (o - hi.astype(jnp.float32)).astype(jnp.bfloat16)
        for i in range(IB):
            for k in range(2):
                rr = slice((2 * p + k) * C, (2 * p + k + 1) * C)
                ll = slice(i * 128, (i + 1) * 128)
                hi_ref[rr, ll] = hi[i * C:(i + 1) * C, k * 128:(k + 1) * 128]
                lo_ref[rr, ll] = lo[i * C:(i + 1) * C, k * 128:(k + 1) * 128]
    wot = wot_ref[...]
    bo = bo_ref[...]
    for q in range(IB // 2):
        ll = slice(q * 256, (q + 1) * 256)
        rt = jnp.dot(wot, hi_ref[:, ll], preferred_element_type=jnp.float32)
        rt = rt + jnp.dot(wot, lo_ref[:, ll], preferred_element_type=jnp.float32)
        for k in range(2):
            i = 2 * q + k
            upd = (rt[:, k * 128:(k + 1) * 128] + bo) * inv_ref[i:i + 1, :]
            out_ref[i] = z_ref[i] + upd.T


def form(at, ball, inv, wot, bo, z):
    return pl.pallas_call(
        form_kernel,
        grid=(JC, ROWS // IB),
        out_shape=jax.ShapeDtypeStruct((ROWS, N, E), jnp.float32),
        in_specs=[
            pl.BlockSpec((IB * C, S), lambda j, i: (i, 0)),
            pl.BlockSpec((1, C, S, 128), lambda j, i: (j, 0, 0, 0)),
            pl.BlockSpec((IB, 128), lambda j, i: (i, j)),
            pl.BlockSpec((E, C * C), lambda j, i: (0, 0)),
            pl.BlockSpec((E, 1), lambda j, i: (0, 0)),
            pl.BlockSpec((IB, 128, E), lambda j, i: (i, j, 0)),
        ],
        out_specs=pl.BlockSpec((IB, 128, E), lambda j, i: (i, j, 0)),
        scratch_shapes=[
            pltpu.VMEM((C * C, IB * 128), jnp.bfloat16),
            pltpu.VMEM((C * C, IB * 128), jnp.bfloat16),
        ],
        compiler_params=pltpu.CompilerParams(vmem_limit_bytes=40 * 1024 * 1024),
        name='form',
    )(at, ball, inv, wot, bo, z)


def solution(mesh):
    rows = P(('data', 'seq', 'dap'), None, None)
    mask_spec = P(('data', 'seq', 'dap'), None)
    pair_spec = P(('data', 'dap'), None, None)

    def device_step(msa, mask, pair, ln_gamma, ln_beta, w_a, b_a, w_b, b_b, w_out, b_out):
        xt = jnp.swapaxes(msa, 1, 2)
        wt = jnp.concatenate([w_a.T, w_b.T], axis=0)
        par = jnp.stack([ln_gamma, ln_beta, jnp.concatenate([b_a, b_b])], axis=1).astype(jnp.float32)
        at, ball, inv, wot = exchange(xt, mask, par, wt, w_out)
        bo = b_out.astype(jnp.float32)[:, None]
        return form(at, ball, inv, wot, bo, pair)

    return jax.shard_map(device_step, mesh=mesh, in_specs=(rows, mask_spec, pair_spec) + (P(),) * 8,
                         out_specs=pair_spec, check_vma=False)
```

```python
import functools

import jax
import jax.numpy as jnp
from jax import lax
from jax.experimental import pallas as pl
from jax.experimental.pallas import tpu as pltpu
from jax.sharding import PartitionSpec as P

MESH = pl.DeviceIdType.MESH
S_LOC, N, K, C, E = 32, 384, 64, 32, 128
S = 256
ROWS = 96
JC = 3
CG = 8
D_VIA_X = 24
IB = 8


def exchange_kernel(x_ref, mask_ref, par_ref, wt_ref, wo_ref,
                    at_ref, ball_ref, inv_ref, wot_ref,
                    stage, ta, ra, rp, mall, atf, wof, ns, ssem, rsem):
    y = lax.axis_index('seq')
    r = lax.axis_index('dap')
    x = r // 2
    c = r % 2
    me = y * 4 + r
    dev_x = (0, y, (1 - x) * 2 + c)
    dev_y = (0, 1 - y, r)
    dev_p = (0, y, x * 2 + 1 - c)
    id_x = y * 4 + (1 - x) * 2 + c
    id_y = (1 - y) * 4 + r
    id_xy = (1 - y) * 4 + (1 - x) * 2 + c
    id_p = y * 4 + x * 2 + 1 - c

    barrier = pltpu.get_barrier_semaphore()
    flips = [(fy, fr) for fy in range(2) for fr in range(4) if fy or fr]
    for fy, fr in flips:
        peer = (0, (y + fy) % 2, (r + fr) % 4)
        pl.semaphore_signal(barrier, inc=1, device_id=peer, device_id_type=MESH)

    gamma, beta, bias = par_ref[:, 0:1], par_ref[:, 1:2], par_ref[:, 2:3]
    wt = wt_ref[...]

    def one_seq(s, carry):
        v = x_ref[s].astype(jnp.float32)
        mean = jnp.sum(v, axis=0, keepdims=True) * (1.0 / K)
        cen = v - mean
        var = jnp.sum(cen * cen, axis=0, keepdims=True) * (1.0 / K)
        xn = (cen * lax.rsqrt(var + 1e-5) * gamma + beta).astype(jnp.bfloat16)
        out = jnp.dot(wt, xn, preferred_element_type=jnp.float32)
        keep = mask_ref[pl.ds(s, 1), :].astype(jnp.float32)
        out = (out + bias) * keep
        for t in range(3):
            stage[t, pl.ds(s, 2 * C, stride=S_LOC), :] = out[:, t * 128:(t + 1) * 128]
        return carry

    lax.fori_loop(0, S_LOC, one_seq, 0, unroll=4)

    my_rows = pl.ds(pl.multiple_of(me * S_LOC, S_LOC), S_LOC)

    for g in range(CG):
        for t in range(3):
            blk = stage[t, g * 128:(g + 1) * 128, :]
            blk = blk.T.astype(jnp.bfloat16)
            lo = t * 128
            while lo < (t + 1) * 128:
                q = lo // ROWS
                hi = min((q + 1) * ROWS, (t + 1) * 128)
                ta[q, g, lo - q * ROWS:hi - q * ROWS, :] = blk[lo - t * 128:hi - t * 128, :]
                lo = hi
    for d in range(C):
        for t in range(JC):
            row = stage[t, (C + d) * S_LOC:(C + d + 1) * S_LOC, :]
            ball_ref[t, d, my_rows, :] = row.astype(jnp.bfloat16)
    mall[my_rows, :] = mask_ref[...].astype(jnp.float32).astype(jnp.bfloat16)

    pl.semaphore_wait(barrier, 7)

    sends = []

    def copy(src, dst, k, dev):
        return pltpu.make_async_remote_copy(
            src_ref=src, dst_ref=dst, send_sem=ssem.at[k], recv_sem=rsem.at[k],
            device_id=dev, device_id_type=MESH)

    def send(src, dst, k, dev):
        cp = copy(src, dst, k, dev)
        cp.start()
        sends.append(cp)

    def arrived(ref, k):
        copy(ref, ref, k, dev_p).wait_recv()

    def rows_of(dev_id):
        return pl.ds(pl.multiple_of(dev_id * S_LOC, S_LOC), S_LOC)

    def b_part(t, dev_id, lo=0, hi=C):
        return ball_ref.at[t, pl.ds(lo, hi - lo), rows_of(dev_id), :]

    A_X, A_Y, A_XY = 0, 1, 2
    A_P = {'o': 3, 'x': 4, 'y': 5, 'd': 6}
    M0 = 7

    def bk(t, what):
        return 14 + t * 9 + ['x', 'y', 'dx', 'dy', 'po', 'px', 'py', 'pdx', 'pdy'].index(what)

    own = 2 * x
    other = 2 * (1 - x)
    send(ta.at[pl.ds(other, 2)], ra.at[0], A_X, dev_x)
    send(ta.at[pl.ds(own, 2)], ra.at[1], A_Y, dev_y)
    send(ta.at[own + 1 - c], rp.at[0], A_P['o'], dev_p)
    for n, (fy, fr) in enumerate(flips):
        peer = (0, (y + fy) % 2, (r + fr) % 4)
        send(mall.at[my_rows], mall.at[my_rows], M0 + n, peer)

    def send_own(t, to):
        dev = {'x': dev_x, 'y': dev_y, 'po': dev_p}[to]
        send(b_part(t, me), b_part(t, me), bk(t, to), dev)

    send_own(0, 'x')
    send_own(0, 'po')

    wof[...] = wo_ref[...].astype(jnp.float32)
    for g in range(CG):
        parts = [wof[pl.ds(4 * g + k, C, stride=C), :] for k in range(4)]
        blk = jnp.concatenate(parts, axis=0)
        wot_ref[:, g * 128:(g + 1) * 128] = blk.T.astype(jnp.bfloat16)

    def got_b(t, frm):
        if frm == 'x':
            arrived(b_part(t, id_x), bk(t, 'x'))
            send(b_part(t, id_x, D_VIA_X, C), b_part(t, id_x, D_VIA_X, C), bk(t, 'dy'), dev_y)
            send(b_part(t, id_x), b_part(t, id_x), bk(t, 'px'), dev_p)
        elif frm == 'y':
            arrived(b_part(t, id_y), bk(t, 'y'))
            send(b_part(t, id_y, 0, D_VIA_X), b_part(t, id_y, 0, D_VIA_X), bk(t, 'dx'), dev_x)
            send(b_part(t, id_y), b_part(t, id_y), bk(t, 'py'), dev_p)
        elif frm == 'dx':
            ref = b_part(t, id_xy, 0, D_VIA_X)
            arrived(ref, bk(t, 'dx'))
            send(ref, ref, bk(t, 'pdx'), dev_p)
        else:
            ref = b_part(t, id_xy, D_VIA_X, C)
            arrived(ref, bk(t, 'dy'))
            send(ref, ref, bk(t, 'pdy'), dev_p)

    arrived(ra.at[0], A_X)
    send(ra.at[0], ra.at[2], A_XY, dev_y)
    send(ra.at[0, 1 - c], rp.at[1], A_P['x'], dev_p)
    send_own(0, 'y')
    send_own(1, 'x')
    arrived(ra.at[1], A_Y)
    send(ra.at[1, 1 - c], rp.at[2], A_P['y'], dev_p)
    got_b(0, 'x')
    send_own(1, 'y')
    send_own(1, 'po')
    send_own(2, 'x')
    arrived(ra.at[2], A_XY)
    send(ra.at[2, 1 - c], rp.at[3], A_P['d'], dev_p)
    got_b(0, 'y')
    send_own(2, 'y')
    send_own(2, 'po')
    for k, name in enumerate(['o', 'x', 'y', 'd']):
        arrived(rp.at[k], A_P[name])

    lane = lax.broadcasted_iota(jnp.int32, (ROWS, 128), 1)
    low = lane < 64
    odd = lax.rem(lane // 32, 2) == 1

    for half in range(2):
        for g in range(CG):
            v = []
            for q in range(4):
                sx, sc = q // 2, q % 2
                same_c = sc == c
                dx = (sx != x).astype(jnp.int32)
                dy = (half != y).astype(jnp.int32)
                slot = dx + 2 * dy
                own_v = ta[r, g].astype(jnp.float32)
                ra_slot = jnp.maximum(slot - 1, 0)
                in_plane = jnp.where(slot == 0, own_v, ra[ra_slot, c, g].astype(jnp.float32))
                v.append(jnp.where(same_c, in_plane, rp[slot, g].astype(jnp.float32)))
            r0, r1, r2, r3 = [pltpu.roll(u, 64, 1) for u in v]
            n0 = jnp.where(low, v[0], r2)
            n1 = jnp.where(low, v[1], r3)
            n2 = jnp.where(low, r0, v[2])
            n3 = jnp.where(low, r1, v[3])
            w0 = jnp.where(odd, pltpu.roll(n1, 32, 1), n0)
            w1 = jnp.where(odd, n1, pltpu.roll(n0, 96, 1))
            w2 = jnp.where(odd, pltpu.roll(n3, 32, 1), n2)
            w3 = jnp.where(odd, n3, pltpu.roll(n2, 96, 1))
            for k, w in enumerate((w0, w1, w2, w3)):
                atf[half, pl.ds(4 * g + k, ROWS, stride=C), :] = w
    for blk in range(12):
        for half in range(2):
            at_ref[half, blk * 256:(blk + 1) * 256, :] = (
                atf[half, blk * 256:(blk + 1) * 256, :].astype(jnp.bfloat16))

    got_b(1, 'x')
    got_b(1, 'y')
    got_b(0, 'dx')
    got_b(0, 'dy')
    got_b(2, 'x')
    got_b(2, 'y')

    for n, (fy, fr) in enumerate(flips):
        frm = ((y - fy + 2) % 2) * 4 + (r - fr + 4) % 4
        arrived(mall.at[rows_of(frm)], M0 + n)
    m = mall[...]
    ns[...] = lax.dot_general(m, m, (((0,), (0,)), ((), ())), preferred_element_type=jnp.float32)
    inv_ref[...] = 1.0 / (1e-3 + ns[pl.ds(pl.multiple_of(r * ROWS, ROWS), ROWS), :])

    for t in (1, 2):
        got_b(t, 'dx')
        got_b(t, 'dy')
    id_px = y * 4 + (1 - x) * 2 + 1 - c
    id_py = (1 - y) * 4 + x * 2 + 1 - c
    id_pd = (1 - y) * 4 + (1 - x) * 2 + 1 - c
    for t in range(JC):
        arrived(b_part(t, id_p), bk(t, 'po'))
        arrived(b_part(t, id_px), bk(t, 'px'))
        arrived(b_part(t, id_py), bk(t, 'py'))
        arrived(b_part(t, id_pd, 0, D_VIA_X), bk(t, 'pdx'))
        arrived(b_part(t, id_pd, D_VIA_X, C), bk(t, 'pdy'))
    for cp in sends:
        cp.wait_send()


def exchange(xt, mask, par, wt, w_out):
    vm = pl.BlockSpec(memory_space=pltpu.VMEM)
    nsem = 14 + 9 * JC
    return pl.pallas_call(
        exchange_kernel,
        out_shape=(
            jax.ShapeDtypeStruct((2, ROWS * C, 128), jnp.bfloat16),
            jax.ShapeDtypeStruct((JC, C, S, 128), jnp.bfloat16),
            jax.ShapeDtypeStruct((ROWS, N), jnp.float32),
            jax.ShapeDtypeStruct((E, C * C), jnp.bfloat16),
        ),
        in_specs=[vm] * 5,
        out_specs=(vm,) * 4,
        scratch_shapes=[
            pltpu.VMEM((3, 2 * C * S_LOC, 128), jnp.float32),
            pltpu.VMEM((4, CG, ROWS, 128), jnp.bfloat16),
            pltpu.VMEM((3, 2, CG, ROWS, 128), jnp.bfloat16),
            pltpu.VMEM((4, CG, ROWS, 128), jnp.bfloat16),
            pltpu.VMEM((S, N), jnp.bfloat16),
            pltpu.VMEM((2, ROWS * C, 128), jnp.float32),
            pltpu.VMEM((C * C, E), jnp.float32),
            pltpu.VMEM((N, N), jnp.float32),
            pltpu.SemaphoreType.DMA((nsem,)),
            pltpu.SemaphoreType.DMA((nsem,)),
        ],
        compiler_params=pltpu.CompilerParams(
            collective_id=0, has_side_effects=True, vmem_limit_bytes=60 * 1024 * 1024),
        name='exchange',
    )(xt, mask, par, wt, w_out)


def first_product(at, rhs_of, hi_ref, lo_ref, slot, p):
    o = jnp.dot(at, rhs_of(p), preferred_element_type=jnp.float32)
    hi = o.astype(jnp.bfloat16)
    lo = (o - hi.astype(jnp.float32)).astype(jnp.bfloat16)
    for i in range(IB):
        for k in range(2):
            rr = slice((2 * p + k) * C, (2 * p + k + 1) * C)
            hi_ref[slot, i, rr, :] = hi[i * C:(i + 1) * C, k * 128:(k + 1) * 128]
            lo_ref[slot, i, rr, :] = lo[i * C:(i + 1) * C, k * 128:(k + 1) * 128]


def second_product(wot, bo, hi_ref, lo_ref, slot, inv_ref, z_ref, out_ref, q):
    a, b = 2 * q, 2 * q + 1
    rt = jnp.dot(wot, jnp.concatenate([hi_ref[slot, a], hi_ref[slot, b]], axis=1),
                 preferred_element_type=jnp.float32)
    rt = rt + jnp.dot(wot, jnp.concatenate([lo_ref[slot, a], lo_ref[slot, b]], axis=1),
                      preferred_element_type=jnp.float32)
    for k, i in enumerate((a, b)):
        upd = (rt[:, k * 128:(k + 1) * 128] + bo) * inv_ref[i:i + 1, :]
        out_ref[i] = z_ref[i] + upd.T


def form_kernel(at_ref, ball_ref, inv_ref, wot_ref, bo_ref, z_ref, out_ref, hi_ref, lo_ref):
    n = pl.program_id(0)
    last = pl.num_programs(0) - 1

    def rhs_of(p):
        return jnp.concatenate([ball_ref[0, 2 * p], ball_ref[0, 2 * p + 1]], axis=1)

    def step(slot, do_first, do_second):
        wot, bo = wot_ref[...], bo_ref[...]
        for p in range(C // 2):
            if do_first:
                at = jnp.concatenate([at_ref[0], at_ref[1]], axis=1)
                first_product(at, rhs_of, hi_ref, lo_ref, slot, p)
            if do_second and p % 4 == 1:
                second_product(wot, bo, hi_ref, lo_ref, 1 - slot, inv_ref, z_ref, out_ref, p // 4)

    for slot in range(2):
        @pl.when((n > 0) & (n < last) & (lax.rem(n, 2) == slot))
        def _():
            step(slot, True, True)

    @pl.when(n == 0)
    def _():
        step(0, True, False)

    @pl.when(n == last)
    def _():
        step((JC * ROWS // IB) % 2, False, True)


def form(at, ball, inv, wot, bo, z):
    ni = ROWS // IB
    steps = JC * ni

    def now(n):
        return jnp.minimum(n, steps - 1)

    def prev(n):
        return jnp.maximum(n - 1, 0)

    return pl.pallas_call(
        form_kernel,
        grid=(steps + 1,),
        out_shape=jax.ShapeDtypeStruct((ROWS, N, E), jnp.float32),
        in_specs=[
            pl.BlockSpec((2, IB * C, 128), lambda n: (0, now(n) % ni, 0)),
            pl.BlockSpec((1, C, S, 128), lambda n: (now(n) // ni, 0, 0, 0)),
            pl.BlockSpec((IB, 128), lambda n: (prev(n) % ni, prev(n) // ni)),
            pl.BlockSpec((E, C * C), lambda n: (0, 0)),
            pl.BlockSpec((E, 1), lambda n: (0, 0)),
            pl.BlockSpec((IB, 128, E), lambda n: (prev(n) % ni, prev(n) // ni, 0)),
        ],
        out_specs=pl.BlockSpec((IB, 128, E), lambda n: (prev(n) % ni, prev(n) // ni, 0)),
        scratch_shapes=[
            pltpu.VMEM((2, IB, C * C, 128), jnp.bfloat16),
            pltpu.VMEM((2, IB, C * C, 128), jnp.bfloat16),
        ],
        compiler_params=pltpu.CompilerParams(vmem_limit_bytes=60 * 1024 * 1024),
        name='form',
    )(at, ball, inv, wot, bo, z)


def solution(mesh):
    rows = P(('data', 'seq', 'dap'), None, None)
    mask_spec = P(('data', 'seq', 'dap'), None)
    pair_spec = P(('data', 'dap'), None, None)

    def device_step(msa, mask, pair, ln_gamma, ln_beta, w_a, b_a, w_b, b_b, w_out, b_out):
        xt = jnp.swapaxes(msa, 1, 2)
        wt = jnp.concatenate([w_a.T, w_b.T], axis=0)
        par = jnp.stack([ln_gamma, ln_beta, jnp.concatenate([b_a, b_b])], axis=1).astype(jnp.float32)
        at, ball, inv, wot = exchange(xt, mask, par, wt, w_out)
        bo = b_out.astype(jnp.float32)[:, None]
        return form(at, ball, inv, wot, bo, pair)

    return jax.shard_map(device_step, mesh=mesh, in_specs=(rows, mask_spec, pair_spec) + (P(),) * 8,
                         out_specs=pair_spec, check_vma=False)
```

```python
import jax
import jax.numpy as jnp
from jax import lax
from jax.experimental import pallas as pl
from jax.experimental.pallas import tpu as pltpu
from jax.sharding import PartitionSpec as P

MESH = pl.DeviceIdType.MESH
L = 128
S_LOC, N, K, C, E = 32, 384, 64, 32, L
S = 256
ROWS = 96
HALF = 48
JC = 3
CG = 8
D_VIA_X = (24, 24, 24)
IB = 8
EARLY = 18
CHUNKS = JC * ROWS // IB
VMEM_LIMIT = 65011712
F32, BF16 = jnp.float32, jnp.bfloat16


def first_product(at_ref, row0, ball_ref, t, hi_ref, lo_ref, slot, p):
    at = jnp.concatenate([at_ref[0, pl.ds(row0, IB * C), :], at_ref[1, pl.ds(row0, IB * C), :]], axis=1)
    rhs = jnp.concatenate([ball_ref[t, 2 * p], ball_ref[t, 2 * p + 1]], axis=1)
    o = jnp.dot(at, rhs, preferred_element_type=F32)
    hi = o.astype(BF16)
    lo = (o - hi.astype(F32)).astype(BF16)
    for i in range(IB):
        for k in range(2):
            rr = slice((2 * p + k) * C, (2 * p + k + 1) * C)
            hi_ref[slot, i, rr, :] = hi[i * C:(i + 1) * C, k * L:(k + 1) * L]
            lo_ref[slot, i, rr, :] = lo[i * C:(i + 1) * C, k * L:(k + 1) * L]


def second_product(wot, bo, hi_ref, lo_ref, slot, inv, z_ref, out_ref, buf, q):
    a, b = 2 * q, 2 * q + 1
    rt = jnp.dot(wot, jnp.concatenate([hi_ref[slot, a], hi_ref[slot, b]], axis=1),
                 preferred_element_type=F32)
    rt = rt + jnp.dot(wot, jnp.concatenate([lo_ref[slot, a], lo_ref[slot, b]], axis=1),
                      preferred_element_type=F32)
    for k, i in enumerate((a, b)):
        upd = (rt[:, k * L:(k + 1) * L] + bo) * inv[i:i + 1, :]
        out_ref[buf[0], buf[1], i] = z_ref[buf[0], buf[1], i] + upd.T


def form_chunks(k0, k1, at_ref, ball_ref, t_base, inv_ref, wot_ref, bo_ref, z_hbm, dst_of,
                hi_ref, lo_ref, zbuf, obuf, zsem, osem, event):
    m0, m1 = k0 // 2, k1 // 2

    def z_copy(k, st, pos):
        i0 = pl.multiple_of(lax.rem(k, 12) * IB, IB)
        j0 = pl.multiple_of((k // 12) * L, L)
        return pltpu.make_async_copy(z_hbm.at[pl.ds(i0, IB), pl.ds(j0, L), :], zbuf.at[st, pos], zsem.at[st, pos])

    def o_copy(k, st, pos):
        return pltpu.make_async_copy(obuf.at[st, pos], dst_of(k), osem.at[st, pos])

    z_copy(k0, lax.rem(m0, 2), 1).start()

    def inv_of(k):
        i0 = pl.multiple_of(lax.rem(k, 12) * IB, IB)
        return inv_ref[k // 12, pl.ds(i0, IB), :]

    def body(m, carry):
        st = lax.rem(m, 2)
        event(m)
        z_copy(2 * m + 1, 1 - st, 0).start()

        @pl.when(m < m1 - 1)
        def _():
            z_copy(2 * m + 2, 1 - st, 1).start()

        @pl.when(m > m0)
        def _():
            z_copy(2 * m - 1, st, 0).wait()

        z_copy(2 * m, st, 1).wait()

        @pl.when(m > m0 + 2)
        def _():
            o_copy(2 * m - 5, st, 0).wait()

        @pl.when(m > m0 + 1)
        def _():
            o_copy(2 * m - 4, st, 1).wait()

        t = m // 6 - t_base
        wot, bo = wot_ref[...], bo_ref[...]
        for slot in range(2):
            k = 2 * m + slot
            row0 = pl.multiple_of(lax.rem(k, 12) * (IB * C), IB * C)
            prev = jnp.maximum(k - 1, k0)
            inv = inv_of(prev)
            for p in range(C // 2):
                first_product(at_ref, row0, ball_ref, t, hi_ref, lo_ref, slot, p)
                if p % 4 == 1:
                    second_product(wot, bo, hi_ref, lo_ref, 1 - slot, inv, zbuf, obuf, (st, slot), p // 4)

        @pl.when(m > m0)
        def _():
            o_copy(2 * m - 1, st, 0).start()

        o_copy(2 * m, st, 1).start()
        return carry

    lax.fori_loop(m0, m1, body, 0)

    st = m1 % 2
    z_copy(k1 - 1, st, 0).wait()
    if m1 - m0 > 2:
        o_copy(2 * m1 - 5, st, 0).wait()
    wot, bo, inv = wot_ref[...], bo_ref[...], inv_of(k1 - 1)
    for q in range(IB // 2):
        second_product(wot, bo, hi_ref, lo_ref, 1, inv, zbuf, obuf, (st, 0), q)
    o_copy(k1 - 1, st, 0).start()
    return [o_copy(2 * m1 - 4, m1 % 2, 1), o_copy(2 * m1 - 3, 1 - st, 0),
            o_copy(2 * m1 - 2, 1 - st, 1), o_copy(k1 - 1, st, 0)]


def exchange_kernel(x_ref, mask_ref, ga_ref, be_ref, wa_ref, ba_ref, wb_ref, bb_ref, wo_ref, bo_in, z_hbm,
                    inv_ref, wot_ref, bo_ref, at_out, b_out, p_out,
                    row_s, keep_s, stage, ta, ra, rp, mall, atf, at_ref, ball_ref, wof, ns,
                    hi_ref, lo_ref, zbuf, obuf, ssem, rsem, zsem, osem, lsem):
    y = lax.axis_index('seq')
    r = lax.axis_index('dap')
    x = r // 2
    c = r % 2
    me = y * 4 + r
    dev_x = (0, y, (1 - x) * 2 + c)
    dev_y = (0, 1 - y, r)
    dev_p = (0, y, x * 2 + 1 - c)
    id_x = y * 4 + (1 - x) * 2 + c
    id_y = (1 - y) * 4 + r
    id_xy = (1 - y) * 4 + (1 - x) * 2 + c
    id_p = y * 4 + x * 2 + 1 - c
    id_px = y * 4 + (1 - x) * 2 + 1 - c
    id_py = (1 - y) * 4 + x * 2 + 1 - c
    id_pd = (1 - y) * 4 + (1 - x) * 2 + 1 - c

    barrier = pltpu.get_barrier_semaphore()
    flips = [(fy, fr) for fy in range(2) for fr in range(4) if fy or fr]
    for fy, fr in flips:
        peer = (0, (y + fy) % 2, (r + fr) % 4)
        pl.semaphore_signal(barrier, inc=1, device_id=peer, device_id_type=MESH)

    def rows_of(dev_id):
        return pl.ds(pl.multiple_of(dev_id * S_LOC, S_LOC), S_LOC)

    my_rows = rows_of(me)
    sends = []

    def copy(src, dst, k, dev):
        return pltpu.make_async_remote_copy(
            src_ref=src, dst_ref=dst, send_sem=ssem.at[k], recv_sem=rsem.at[k],
            device_id=dev, device_id_type=MESH)

    def send(refs, k, dev):
        copy(*refs(), k, dev).start()
        sends.append(lambda: copy(*refs(), k, dev).wait_send())

    def arrived(ref, k):
        copy(ref, ref, k, dev_p).wait_recv()

    def b_part(t, dev_id, lo=0, hi=C):
        return ball_ref.at[t, pl.ds(lo, hi - lo), rows_of(dev_id), :]

    def ak(h, what):
        return h * 7 + ['x', 'y', 'd', 'po', 'px', 'py', 'pd'].index(what)

    M0 = 14

    def bk(t, what):
        return 21 + t * 9 + ['x', 'y', 'dx', 'dy', 'po', 'px', 'py', 'pdx', 'pdy'].index(what)

    def send_b(t, *to):
        for w in to:
            dev = {'x': dev_x, 'y': dev_y, 'po': dev_p}[w]
            send(lambda: (b_part(t, me),) * 2, bk(t, w), dev)

    def got_b(t, *frm):
        v = D_VIA_X[t]
        for w in frm:
            if w == 'x':
                arrived(b_part(t, id_x), bk(t, 'x'))
                send(lambda: (b_part(t, id_x, v, C),) * 2, bk(t, 'dy'), dev_y)
                send(lambda: (b_part(t, id_x),) * 2, bk(t, 'px'), dev_p)
            elif w == 'y':
                arrived(b_part(t, id_y), bk(t, 'y'))
                send(lambda: (b_part(t, id_y, 0, v),) * 2, bk(t, 'dx'), dev_x)
                send(lambda: (b_part(t, id_y),) * 2, bk(t, 'py'), dev_p)
            elif w == 'dx':
                arrived(b_part(t, id_xy, 0, v), bk(t, 'dx'))
                send(lambda: (b_part(t, id_xy, 0, v),) * 2, bk(t, 'pdx'), dev_p)
            else:
                arrived(b_part(t, id_xy, v, C), bk(t, 'dy'))
                send(lambda: (b_part(t, id_xy, v, C),) * 2, bk(t, 'pdy'), dev_p)

    def got_b_partner(t):
        v = D_VIA_X[t]
        arrived(b_part(t, id_p), bk(t, 'po'))
        arrived(b_part(t, id_px), bk(t, 'px'))
        arrived(b_part(t, id_py), bk(t, 'py'))
        arrived(b_part(t, id_pd, 0, v), bk(t, 'pdx'))
        arrived(b_part(t, id_pd, v, C), bk(t, 'pdy'))

    own, other = 2 * x, 2 * (1 - x)

    def got_a(h, w):
        n = 'xyd'.index(w)
        arrived(ra.at[n, h], ak(h, w))
        if w == 'x':
            send(lambda: (ra.at[0, h], ra.at[2, h]), ak(h, 'd'), dev_y)
        send(lambda: (ra.at[n, h, 1 - c], rp.at[n + 1, h]), ak(h, 'p' + w), dev_p)

    row_s[0:1, 0:64] = ga_ref[...].astype(F32)
    row_s[0:1, 64:L] = be_ref[...].astype(F32)
    row_s[1:2, 0:32] = ba_ref[...].astype(F32)
    row_s[1:2, 32:64] = bb_ref[...].astype(F32)
    row_s[1:2, 64:L] = jnp.zeros((1, 64), F32)
    cols = jnp.broadcast_to(row_s[0:1, :], (L, L)).T
    gamma, beta = cols[0:64, :], cols[64:L, :]
    bias = jnp.broadcast_to(row_s[1:2, :], (L, L)).T[0:64, :]
    wt = jnp.concatenate([wa_ref[...], wb_ref[...]], axis=0)
    mall[my_rows, :] = mask_ref[...].astype(F32).astype(BF16)
    for t in range(JC):
        keep_s[t] = mask_ref[:, t * L:(t + 1) * L].astype(F32)

    def project(t):
        ll = slice(t * L, (t + 1) * L)

        def two_seqs(s2, carry):
            xs = []
            for u in range(2):
                v = x_ref[2 * s2 + u, :, ll].astype(F32)
                mean = jnp.sum(v, axis=0, keepdims=True) * (1.0 / K)
                cen = v - mean
                var = jnp.sum(cen * cen, axis=0, keepdims=True) * (1.0 / K)
                xs.append((cen * lax.rsqrt(var + 1e-5) * gamma + beta).astype(BF16))
            out = jnp.dot(wt, jnp.concatenate(xs, axis=1), preferred_element_type=F32)
            for u in range(2):
                keep = keep_s[t, pl.ds(2 * s2 + u, 1), :]
                stage[t, pl.ds(2 * s2 + u, 2 * C, stride=S_LOC), :] = (out[:, u * L:(u + 1) * L] + bias) * keep
            return carry

        lax.fori_loop(0, S_LOC // 2, two_seqs, 0, unroll=4)
        for d in range(C):
            ball_ref[t, d, my_rows, :] = stage[t, (C + d) * S_LOC:(C + d + 1) * S_LOC, :].astype(BF16)
        for g in range(CG):
            blk = stage[t, g * L:(g + 1) * L, :].T.astype(BF16)
            lo = t * L
            while lo < (t + 1) * L:
                q = lo // HALF
                hi = min((q + 1) * HALF, (t + 1) * L)
                ta[q // 2, q % 2, g, lo - q * HALF:hi - q * HALF, :] = blk[lo - t * L:hi - t * L, :]
                lo = hi

    project(0)
    pl.semaphore_wait(barrier, 7)
    send_b(0, 'x', 'y', 'po')
    for n, (fy, fr) in enumerate(flips):
        peer = (0, (y + fy) % 2, (r + fr) % 4)
        send(lambda: (mall.at[my_rows],) * 2, M0 + n, peer)
    project(1)
    project(2)
    for h in range(2):
        send(lambda h=h: (ta.at[own + 1 - c, h], rp.at[0, h]), ak(h, 'po'), dev_p)
    send(lambda: (ta.at[pl.ds(other, 2), 0], ra.at[0, 0]), ak(0, 'x'), dev_x)
    send(lambda: (ta.at[pl.ds(own, 2), 0], ra.at[1, 0]), ak(0, 'y'), dev_y)

    wof[...] = wo_ref[...].astype(F32)
    for g in range(CG):
        parts = [wof[pl.ds(4 * g + k, C, stride=C), :] for k in range(4)]
        wot_ref[:, g * L:(g + 1) * L] = jnp.concatenate(parts, axis=0).T.astype(BF16)
    bo_ref[...] = jnp.broadcast_to(bo_in[...].astype(F32), (E, E)).T

    got_b(0, 'x', 'y')
    send(lambda: (ta.at[pl.ds(other, 2), 1], ra.at[0, 1]), ak(1, 'x'), dev_x)

    for n, (fy, fr) in enumerate(flips):
        frm = ((y - fy + 2) % 2) * 4 + (r - fr + 4) % 4
        arrived(mall.at[rows_of(frm)], M0 + n)
    mm = mall[...]
    ns[...] = lax.dot_general(mm, mm, (((0,), (0,)), ((), ())), preferred_element_type=F32)
    for t in range(JC):
        inv_ref[t] = 1.0 / (1e-3 + ns[pl.ds(pl.multiple_of(r * ROWS, 32), ROWS), t * L:(t + 1) * L])

    got_a(0, 'x')
    send(lambda: (ta.at[pl.ds(own, 2), 1], ra.at[1, 1]), ak(1, 'y'), dev_y)
    send_b(1, 'x', 'po')
    got_a(0, 'y')
    got_b(0, 'dy', 'dx')
    got_a(0, 'd')

    lane = lax.broadcasted_iota(jnp.int32, (HALF, L), 1)
    low = lane < 64
    odd = lax.rem(lane // 32, 2) == 1

    def left_operand(h):
        for n in range(4):
            arrived(rp.at[n, h], ak(h, 'p' + 'oxyd'[n]))
        for half in range(2):
            for g in range(CG):
                v = []
                for q in range(4):
                    sx, sc = q // 2, q % 2
                    slot = (sx != x).astype(jnp.int32) + 2 * (half != y).astype(jnp.int32)
                    own_v = ta[r, h, g].astype(F32)
                    far_v = ra[jnp.maximum(slot - 1, 0), h, c, g].astype(F32)
                    in_plane = jnp.where(slot == 0, own_v, far_v)
                    v.append(jnp.where(sc == c, in_plane, rp[slot, h, g].astype(F32)))
                r0, r1, r2, r3 = [pltpu.roll(u, 64, 1) for u in v]
                n0 = jnp.where(low, v[0], r2)
                n1 = jnp.where(low, v[1], r3)
                n2 = jnp.where(low, r0, v[2])
                n3 = jnp.where(low, r1, v[3])
                w0 = jnp.where(odd, pltpu.roll(n1, 32, 1), n0)
                w1 = jnp.where(odd, n1, pltpu.roll(n0, 96, 1))
                w2 = jnp.where(odd, pltpu.roll(n3, 32, 1), n2)
                w3 = jnp.where(odd, n3, pltpu.roll(n2, 96, 1))
                for k, w in enumerate((w0, w1, w2, w3)):
                    atf[half, pl.ds(4 * g + k, HALF, stride=C), :] = w
        hc = HALF * C
        for half in range(2):
            for blk in range(6):
                at_ref[half, h * hc + blk * 256:h * hc + (blk + 1) * 256, :] = (
                    atf[half, blk * 256:(blk + 1) * 256, :].astype(BF16))

    left_operand(0)
    got_b_partner(0)

    at_copy = pltpu.make_async_copy(at_ref, at_out, lsem.at[0])
    b_copy = [pltpu.make_async_copy(ball_ref.at[t], b_out.at[t - 1], lsem.at[t]) for t in (1, 2)]

    def event(m):
        @pl.when(m == 1)
        def _():
            got_a(1, 'x')
            send_b(1, 'y')
            send_b(2, 'x', 'po')
            got_a(1, 'y')

        @pl.when(m == 3)
        def _():
            got_b(1, 'x')
            send_b(2, 'y')
            got_a(1, 'd')
            left_operand(1)
            at_copy.start()

        @pl.when(m == 5)
        def _():
            got_b(1, 'y')
            got_b(2, 'x')

        @pl.when(m == 6)
        def _():
            got_b(1, 'dx', 'dy')
            got_b_partner(1)
            b_copy[0].start()

        @pl.when(m == 7)
        def _():
            got_b(2, 'y')

        @pl.when(m == 8)
        def _():
            got_b(2, 'dy')

    outs = form_chunks(0, EARLY, at_ref, ball_ref, 0, inv_ref, wot_ref, bo_ref, z_hbm,
                       lambda k: p_out.at[pl.ds(pl.multiple_of(k * IB, IB), IB)],
                       hi_ref, lo_ref, zbuf, obuf, zsem, osem, event)
    got_b(2, 'dx')
    got_b_partner(2)
    b_copy[1].start()
    for sent in sends:
        sent()
    for cp in outs:
        cp.wait()
    at_copy.wait()
    for cp in b_copy:
        cp.wait()


def exchange(xt, mask, ga, be, wa, ba, wb, bb, w_out, bo, z):
    vm = pl.BlockSpec(memory_space=pltpu.VMEM)
    hbm = pl.BlockSpec(memory_space=pl.ANY)
    nsem = 21 + 9 * JC
    return pl.pallas_call(
        exchange_kernel,
        out_shape=(
            jax.ShapeDtypeStruct((JC, ROWS, L), F32),
            jax.ShapeDtypeStruct((E, C * C), BF16),
            jax.ShapeDtypeStruct((E, E), F32),
            jax.ShapeDtypeStruct((2, ROWS * C, L), BF16),
            jax.ShapeDtypeStruct((2, C, S, L), BF16),
            jax.ShapeDtypeStruct((EARLY * IB, L, E), F32),
        ),
        in_specs=[vm] * 10 + [hbm],
        out_specs=(vm,) * 3 + (hbm,) * 3,
        scratch_shapes=[
            pltpu.VMEM((8, L), F32),
            pltpu.VMEM((JC, S_LOC, L), F32),
            pltpu.VMEM((JC, 2 * C * S_LOC, L), F32),
            pltpu.VMEM((4, 2, CG, HALF, L), BF16),
            pltpu.VMEM((3, 2, 2, CG, HALF, L), BF16),
            pltpu.VMEM((4, 2, CG, HALF, L), BF16),
            pltpu.VMEM((S, N), BF16),
            pltpu.VMEM((2, HALF * C, L), F32),
            pltpu.VMEM((2, ROWS * C, L), BF16),
            pltpu.VMEM((JC, C, S, L), BF16),
            pltpu.VMEM((C * C, E), F32),
            pltpu.VMEM((N, N), F32),
            pltpu.VMEM((2, IB, C * C, L), BF16),
            pltpu.VMEM((2, IB, C * C, L), BF16),
            pltpu.VMEM((2, 2, IB, L, E), F32),
            pltpu.VMEM((2, 2, IB, L, E), F32),
            pltpu.SemaphoreType.DMA((nsem,)),
            pltpu.SemaphoreType.DMA((nsem,)),
            pltpu.SemaphoreType.DMA((2, 2)),
            pltpu.SemaphoreType.DMA((2, 2)),
            pltpu.SemaphoreType.DMA((3,)),
        ],
        compiler_params=pltpu.CompilerParams(
            collective_id=0, has_side_effects=True, vmem_limit_bytes=VMEM_LIMIT),
        name='exchange',
    )(xt, mask, ga, be, wa, ba, wb, bb, w_out, bo, z)


def form_kernel(inv_ref, wot_ref, bo_ref, at_hbm, b_hbm, p_hbm, z_hbm, out_hbm,
                at_ref, ball_ref, pbuf, hi_ref, lo_ref, zbuf, obuf, zsem, osem, lsem, psem):
    at_copy = pltpu.make_async_copy(at_hbm, at_ref, lsem.at[0])
    b_copy = [pltpu.make_async_copy(b_hbm.at[t], ball_ref.at[t], lsem.at[1 + t]) for t in range(2)]
    at_copy.start()
    b_copy[0].start()
    b_copy[1].start()

    units = EARLY // 6
    u_rows = 6 * IB
    p_in = [pltpu.make_async_copy(p_hbm.at[pl.ds(u * u_rows, u_rows)], pbuf.at[u], psem.at[0, u])
            for u in range(units)]
    p_out = [pltpu.make_async_copy(
        pbuf.at[u], out_hbm.at[pl.ds((u % 2) * u_rows, u_rows), pl.ds((u // 2) * L, L), :], psem.at[1, u])
        for u in range(units)]

    def dst_of(k):
        i0 = pl.multiple_of(lax.rem(k, 12) * IB, IB)
        j0 = pl.multiple_of((k // 12) * L, L)
        return out_hbm.at[pl.ds(i0, IB), pl.ds(j0, L), :]

    m0 = EARLY // 2

    def event(m):
        for u in range(units):
            @pl.when(m == m0 + 1 + u)
            def _():
                p_in[u].start()

            @pl.when(m == m0 + 3 + u)
            def _():
                p_in[u].wait()
                p_out[u].start()

        @pl.when(m == m0 + 3)
        def _():
            b_copy[1].wait()

    at_copy.wait()
    b_copy[0].wait()
    outs = form_chunks(EARLY, CHUNKS, at_ref, ball_ref, 1, inv_ref, wot_ref, bo_ref, z_hbm, dst_of,
                       hi_ref, lo_ref, zbuf, obuf, zsem, osem, event)
    for cp in outs + p_out:
        cp.wait()


def form(inv, wot, bo, at, ball, part, z):
    vm = pl.BlockSpec(memory_space=pltpu.VMEM)
    hbm = pl.BlockSpec(memory_space=pl.ANY)
    return pl.pallas_call(
        form_kernel,
        out_shape=jax.ShapeDtypeStruct((ROWS, N, E), F32),
        in_specs=[vm] * 3 + [hbm] * 4,
        out_specs=hbm,
        scratch_shapes=[
            pltpu.VMEM((2, ROWS * C, L), BF16),
            pltpu.VMEM((2, C, S, L), BF16),
            pltpu.VMEM((EARLY // 6, 6 * IB, L, E), F32),
            pltpu.VMEM((2, IB, C * C, L), BF16),
            pltpu.VMEM((2, IB, C * C, L), BF16),
            pltpu.VMEM((2, 2, IB, L, E), F32),
            pltpu.VMEM((2, 2, IB, L, E), F32),
            pltpu.SemaphoreType.DMA((2, 2)),
            pltpu.SemaphoreType.DMA((2, 2)),
            pltpu.SemaphoreType.DMA((3,)),
            pltpu.SemaphoreType.DMA((2, EARLY // 6)),
        ],
        compiler_params=pltpu.CompilerParams(vmem_limit_bytes=VMEM_LIMIT),
        name='form',
    )(inv, wot, bo, at, ball, part, z)


def solution(mesh):
    rows = P(('data', 'seq', 'dap'), None, None)
    mask_spec = P(('data', 'seq', 'dap'), None)
    pair_spec = P(('data', 'dap'), None, None)

    def device_step(msa, mask, pair, ln_gamma, ln_beta, w_a, b_a, w_b, b_b, w_out, b_out):
        inv, wot, bo, at, ball, part = exchange(
            jnp.swapaxes(msa, 1, 2), mask, ln_gamma[None], ln_beta[None], w_a.T, b_a[None], w_b.T, b_b[None],
            w_out, b_out[None], pair)
        return form(inv, wot, bo, at, ball, part, pair)

    return jax.shard_map(device_step, mesh=mesh, in_specs=(rows, mask_spec, pair_spec) + (P(),) * 8,
                         out_specs=pair_spec, check_vma=False)
```
